32 devices in a mesh: stage: 4 (over y, z), data: 8 (over x, core).
Axes of the slice: x: 4, y: 2, z: 2, core: 2. Of those that a mesh axis runs over, the one named last changes fastest.
The devices are a block of a 4x4x8 slice.
Arguments:
- w_master: float32 [192, 512, 512], P('stage', 'data'), parts along dimension 0
- momentum: float32 [192, 512, 512], P('stage', 'data'), parts along dimension 0
- grads: bfloat16 [32, 48, 512, 512], P(('stage', 'data')), parts along dimension 0
Outputs:
- output 1: float32 [192, 512, 512], P('stage', 'data'), parts along dimension 0
- output 2: float32 [192, 512, 512], P('stage', 'data'), parts along dimension 0
There are 4 independent parts. The reference program is written for one: setup_inputs(seed, part) draws one part's arguments, and reference() takes and returns one part's arrays. A program takes and returns all parts, laid end to end along the dimension named above; each array names one.
All inputs are finite; a program needn't handle non-finite values.
Results may differ from the reference program's by a relative error of at most 0.0147327.
Values are sent between devices in bfloat16 or wider.
A program may use at most 768 MiB of HBM per device.

```python
import math
import jax
import jax.numpy as jnp
from jax import lax

GROUP_SIZE = 8
NUM_MATS = 48
MAT_ROWS = 512
MAT_COLS = 512
NS_ITERS = 5

MOMENTUM_COEF = 0.95
LEARN_RATE = 0.05
WEIGHT_DECAY = 0.2
NORM_EPS = 1e-7
COEF_A = 3.4445
COEF_B = -4.7750
COEF_C = 2.0315
RMS_SCALE = 0.2 * math.sqrt(max(MAT_ROWS, MAT_COLS))


def setup_inputs(seed: int = 0, part: int = 0) -> dict:
    base_key = jax.random.fold_in(jax.random.key(seed), part)
    sub_keys = jax.random.split(base_key, 6)
    mat_shape = (NUM_MATS, MAT_ROWS, MAT_COLS)
    w_master = 0.02 * jax.random.normal(sub_keys[0], mat_shape, jnp.float32)
    noise_base = jax.random.normal(sub_keys[1], mat_shape, jnp.float32)
    low_left = jax.random.normal(sub_keys[2], (NUM_MATS, MAT_ROWS, 4), jnp.float32)
    low_right = jax.random.normal(sub_keys[3], (NUM_MATS, 4, MAT_COLS), jnp.float32)
    shared = 0.25 * jnp.einsum('mrk,mkc->mrc', low_left, low_right)
    row_scale = jax.random.uniform(sub_keys[4], (NUM_MATS, MAT_ROWS, 1), jnp.float32, 0.5, 1.5)
    momentum = row_scale * (noise_base + shared)
    grads = (jax.random.normal(sub_keys[5], (GROUP_SIZE,) + mat_shape, jnp.float32) * GROUP_SIZE ** -0.5).astype(jnp.bfloat16)
    return {'w_master': w_master, 'momentum': momentum, 'grads': grads}


def newton_schulz(x_start):
    is_tall = MAT_ROWS > MAT_COLS
    x_cur = x_start.T if is_tall else x_start
    for _ in range(NS_ITERS):
        gram_mat = jnp.dot(x_cur, x_cur.T, preferred_element_type=jnp.float32).astype(jnp.bfloat16)
        gram_sq = jnp.dot(gram_mat, gram_mat, preferred_element_type=jnp.float32)
        poly_mat = (COEF_B * gram_mat.astype(jnp.float32) + COEF_C * gram_sq).astype(jnp.bfloat16)
        poly_x = jnp.dot(poly_mat, x_cur, preferred_element_type=jnp.float32)
        x_cur = (COEF_A * x_cur.astype(jnp.float32) + poly_x).astype(jnp.bfloat16)
    return x_cur.T if is_tall else x_cur


def reference(w_master, momentum, grads):
    grad_sum = jnp.sum(grads.astype(jnp.float32), axis=0)
    mom_new = MOMENTUM_COEF * momentum + grad_sum
    frob_norm = jnp.sqrt(jnp.sum(mom_new * mom_new, axis=(1, 2)))

    def one_matrix(mat_pair):
        mom_one, norm_one = mat_pair
        x_start = (mom_one.astype(jnp.bfloat16).astype(jnp.float32) / (norm_one + NORM_EPS)).astype(jnp.bfloat16)
        return newton_schulz(x_start)

    x_ortho = lax.map(one_matrix, (mom_new, frob_norm))
    w_new = w_master - LEARN_RATE * (x_ortho.astype(jnp.float32) * RMS_SCALE + WEIGHT_DECAY * w_master)
    return w_new, mom_new
```

```python
import functools
import math
import jax
import jax.numpy as jnp
from jax import lax
from jax.experimental import pallas as pl
from jax.experimental.pallas import tpu as pltpu
from jax.sharding import PartitionSpec as P

MOMENTUM_COEF = 0.95
LEARN_RATE = 0.05
WEIGHT_DECAY = 0.2
NORM_EPS = 1e-7
COEF_A = 3.4445
COEF_B = -4.7750
COEF_C = 2.0315
NS_ITERS = 5
F32 = jnp.float32
BF16 = jnp.bfloat16


def muon_kernel(G, R, g_ref, w_ref, m_ref, wn_ref, mn_ref,
                rl, orl, fo, fi, dr, po, ow, mi, mo, mb, mr, nso, nr, xo, orr, wi, wo, a_s, b_s,
                s_rl, s_fi, s_dr, s_po, s_mr, s_nr, s_or,
                t_raw, t_fo, t_m, t_n, t_o,
                l_rl, l_ow, l_m, l_w, l_mo, l_wo):
    NM = G
    RB = mi.shape[2]
    H = RB // 2
    C = mi.shape[3]
    scale = 0.2 * math.sqrt(max(G * RB, C))
    chips = G // 2
    d = lax.axis_index('data')
    p = d // 2
    c = lax.rem(d, 2)
    right = lax.rem(p + 1, chips)
    left = lax.rem(p + chips - 1, chips)
    opp = lax.rem(p + 2, chips)
    partner = 2 * p + (1 - c)

    def remote(src, dst, ssem, rsem, dev):
        pltpu.make_async_remote_copy(src_ref=src, dst_ref=dst, send_sem=ssem, recv_sem=rsem,
                                     device_id={'data': dev}, device_id_type=pl.DeviceIdType.MESH).start()

    def drain(ref, sem):
        pltpu.make_async_copy(ref, ref, sem).wait()

    def mats(r):
        return pl.ds(r * NM, NM)

    def grows(r, dev, half):
        return g_ref.at[mats(r), pl.ds(pl.multiple_of(dev * RB + half * H, H), H), :]

    def load_relay(r):
        s = r % 2
        pltpu.make_async_copy(grows(r, 2 * right + c, 0), orl.at[s, 0], l_rl.at[r]).start()
        pltpu.make_async_copy(grows(r, 2 * left + c, 1), orl.at[s, 1], l_rl.at[r]).start()

    def load_final(r):
        s = r % 2
        pltpu.make_async_copy(g_ref.at[mats(r), pl.ds(pl.multiple_of(d * RB, RB), RB), :], ow.at[s], l_ow.at[r]).start()
        pltpu.make_async_copy(m_ref.at[mats(r)], mi.at[s], l_m.at[r]).start()

    def load_w(r):
        pltpu.make_async_copy(w_ref.at[mats(r)], wi.at[r % 2], l_w.at[r]).start()

    def raw(r):
        for cc in range(2):
            remote(grows(r, 2 * opp + cc, 0), rl.at[r, 0, c], t_raw.at[r], s_rl.at[r, 0], 2 * right + cc)
            remote(grows(r, 2 * opp + cc, 1), rl.at[r, 1, c], t_raw.at[r], s_rl.at[r, 1], 2 * left + cc)
        remote(grows(r, 2 * right + (1 - c), 0), rl.at[r, 0, 2], t_raw.at[r], s_rl.at[r, 0], partner)
        remote(grows(r, 2 * left + (1 - c), 1), rl.at[r, 1, 2], t_raw.at[r], s_rl.at[r, 1], partner)
        for cc in range(2):
            remote(grows(r, 2 * right + cc, 1), dr.at[r, 0, c], t_raw.at[r], s_dr.at[r], 2 * right + cc)
            remote(grows(r, 2 * left + cc, 0), dr.at[r, 1, c], t_raw.at[r], s_dr.at[r], 2 * left + cc)
        remote(g_ref.at[mats(r), pl.ds(pl.multiple_of(partner * RB, RB), RB), :], po.at[r], t_raw.at[r], s_po.at[r], partner)

    def relay(r):
        s = r % 2
        drain(orl.at[s], l_rl.at[r])
        for q in range(2):
            drain(rl.at[r, q], s_rl.at[r, q])
            if r >= 2:
                drain(fo.at[s, q], t_fo.at[r - 2, q])

            def body(k, _):
                fo[s, q, k] = ((rl[r, q, 0, k].astype(F32) + rl[r, q, 1, k].astype(F32))
                               + (rl[r, q, 2, k].astype(F32) + orl[s, q, k].astype(F32)))
                return 0
            lax.fori_loop(0, NM, body, 0)
            remote(fo.at[s, q], fi.at[r, q], t_fo.at[r, q], s_fi.at[r, q], 2 * (right if q == 0 else left) + c)
        if r + 2 < R:
            load_relay(r + 2)

    def final(r):
        s = r % 2
        drain(ow.at[s], l_ow.at[r])
        drain(mi.at[s], l_m.at[r])
        drain(po.at[r], s_po.at[r])
        drain(dr.at[r], s_dr.at[r])
        for q in range(2):
            drain(fi.at[r, q], s_fi.at[r, q])
        if r >= 2:
            drain(mo.at[s], l_mo.at[r - 2])

        def body(k, _):
            part = jnp.zeros((8, 128), F32)
            for q in range(2):
                rows = pl.ds(q * H, H)
                grad = ((dr[r, 1 - q, 0, k].astype(F32) + dr[r, 1 - q, 1, k].astype(F32))
                        + (po[r, k, rows, :].astype(F32) + ow[s, k, rows, :].astype(F32))) + fi[r, q, k]
                new = MOMENTUM_COEF * mi[s, k, rows, :] + grad
                mo[s, k, rows, :] = new
                mb[r, k, rows, :] = new.astype(BF16)
                sq = jnp.sum((new * new).reshape(H // 8, 8, C), axis=0)
                for j in range(C // 128):
                    part = part + sq[:, j * 128:(j + 1) * 128]
            nso[r, k] = part
            return 0
        lax.fori_loop(0, NM, body, 0)
        mine = pl.ds(pl.multiple_of(d * RB, RB), RB)
        for j in range(1, G):
            dev = lax.rem(d + j, G)
            remote(nso.at[r, dev], nr.at[r, d], t_n.at[r], s_nr.at[r], dev)
            remote(mb.at[r, dev], mr.at[r, mine, :], t_m.at[r], s_mr.at[r], dev)
        mr[r, mine, :] = mb[r, d]
        nr[r, d] = nso[r, d]
        pltpu.make_async_copy(mo.at[s], mn_ref.at[mats(r)], l_mo.at[r]).start()
        if r + 2 < R:
            load_final(r + 2)

    def ns(r):
        drain(nr.at[r, pl.ds(0, G - 1)], s_nr.at[r])
        drain(mr.at[r, pl.ds(0, (G - 1) * RB), :], s_mr.at[r])
        tot = jnp.sum(jnp.sum(nr[r], axis=0), axis=(0, 1), keepdims=True)
        denom = jnp.sqrt(tot) + NORM_EPS

        def init(k, _):
            rows = pl.ds(pl.multiple_of(k * RB, RB), RB)
            xo[r, rows, :] = (mr[r, rows, :].astype(F32) / denom).astype(BF16)
            return 0
        lax.fori_loop(0, G, init, 0)

        def step(_, carry):
            x = xo[r]
            a_s[...] = lax.dot_general(x, x, (((1,), (1,)), ((), ())), preferred_element_type=F32).astype(BF16)
            a = a_s[...]
            b_s[...] = (COEF_B * a.astype(F32) + COEF_C * jnp.dot(a, a, preferred_element_type=F32)).astype(BF16)
            xo[r] = (COEF_A * x.astype(F32) + jnp.dot(b_s[...], x, preferred_element_type=F32)).astype(BF16)
            return carry
        lax.fori_loop(0, NS_ITERS, step, 0)
        for j in range(1, G):
            dev = lax.rem(d + j, G)
            remote(xo.at[r, pl.ds(pl.multiple_of(dev * RB, RB), RB), :], orr.at[r, d], t_o.at[r], s_or.at[r], dev)
        orr[r, d] = xo[r, pl.ds(pl.multiple_of(d * RB, RB), RB), :]

    def wupd(r):
        s = r % 2
        drain(wi.at[s], l_w.at[r])
        drain(orr.at[r, pl.ds(0, G - 1)], s_or.at[r])
        if r >= 2:
            drain(wo.at[s], l_wo.at[r - 2])

        def body(k, _):
            w = wi[s, k]
            wo[s, k] = w - LEARN_RATE * (orr[r, k].astype(F32) * scale + WEIGHT_DECAY * w)
            return 0
        lax.fori_loop(0, NM, body, 0)
        pltpu.make_async_copy(wo.at[s], wn_ref.at[mats(r)], l_wo.at[r]).start()
        if r + 2 < R:
            load_w(r + 2)

    bar = pltpu.get_barrier_semaphore()
    for j in range(1, G):
        pl.semaphore_signal(bar, inc=1, device_id={'data': lax.rem(d + j, G)}, device_id_type=pl.DeviceIdType.MESH)
    pl.semaphore_wait(bar, G - 1)

    for r in range(min(2, R)):
        raw(r)
        load_relay(r)
        load_final(r)
        load_w(r)
    for r in range(R + 3):
        if r < R:
            relay(r)
        if r + 2 < R:
            raw(r + 2)
        if 0 <= r - 1 < R:
            final(r - 1)
        if 0 <= r - 2 < R:
            ns(r - 2)
        if 0 <= r - 3 < R:
            wupd(r - 3)
    for r in range(R):
        drain(g_ref.at[pl.ds(0, 6)], t_raw.at[r])
        drain(mb.at[r, pl.ds(0, G - 1)], t_m.at[r])
        drain(nso.at[r, pl.ds(0, G - 1)], t_n.at[r])
        drain(xo.at[r, pl.ds(0, (G - 1) * RB), :], t_o.at[r])
        if r >= R - 2:
            for q in range(2):
                drain(fo.at[r % 2, q], t_fo.at[r, q])
            drain(mo.at[r % 2], l_mo.at[r])
            drain(wo.at[r % 2], l_wo.at[r])


def solution(mesh):
    G = mesh.shape['data']
    row_spec = P('stage', 'data', None)
    grad_spec = P(('stage', 'data'), None, None, None)

    def local_step(w_rows, mom_rows, grad_full):
        n_mats, RB, C = w_rows.shape
        NM = G
        R = n_mats // NM
        H = RB // 2
        N = G * RB
        assert R * NM == n_mats and grad_full.shape[1:] == (n_mats, N, C) and N == C and G == 8
        dma = pltpu.SemaphoreType.DMA
        vm = pltpu.VMEM
        any_spec = pl.BlockSpec(memory_space=pl.ANY)
        out = jax.ShapeDtypeStruct(w_rows.shape, F32)
        w_new, mom_new = pl.pallas_call(
            functools.partial(muon_kernel, G, R),
            out_shape=(out, out),
            in_specs=[any_spec] * 3,
            out_specs=(any_spec, any_spec),
            scratch_shapes=[
                vm((R, 2, 3, NM, H, C), BF16),
                vm((2, 2, NM, H, C), BF16),
                vm((2, 2, NM, H, C), F32),
                vm((R, 2, NM, H, C), F32),
                vm((R, 2, 2, NM, H, C), BF16),
                vm((R, NM, RB, C), BF16),
                vm((2, NM, RB, C), BF16),
                vm((2, NM, RB, C), F32),
                vm((2, NM, RB, C), F32),
                vm((R, NM, RB, C), BF16),
                vm((R, N, C), BF16),
                vm((R, NM, 8, 128), F32),
                vm((R, NM, 8, 128), F32),
                vm((R, N, C), BF16),
                vm((R, NM, RB, C), BF16),
                vm((2, NM, RB, C), F32),
                vm((2, NM, RB, C), F32),
                vm((N, N), BF16),
                vm((N, N), BF16),
                dma((R, 2)), dma((R, 2)), dma((R,)), dma((R,)), dma((R,)), dma((R,)), dma((R,)),
                dma((R,)), dma((R, 2)), dma((R,)), dma((R,)), dma((R,)),
                dma((R,)), dma((R,)), dma((R,)), dma((R,)), dma((R,)), dma((R,)),
            ],
            compiler_params=pltpu.CompilerParams(collective_id=0, has_side_effects=True, vmem_limit_bytes=67043328),
            cost_estimate=pl.CostEstimate(flops=R * NS_ITERS * 6 * N * N * C, bytes_accessed=100 * 2 ** 20, transcendentals=0),
            name='muon',
        )(grad_full[0], w_rows, mom_rows)
        return w_new, mom_new

    return jax.shard_map(local_step, mesh=mesh, in_specs=(row_spec, row_spec, grad_spec), out_specs=(row_spec, row_spec), check_vma=False)
```

```python
import functools
import math
import jax
import jax.numpy as jnp
from jax import lax
from jax.experimental import pallas as pl
from jax.experimental.pallas import tpu as pltpu
from jax.sharding import PartitionSpec as P

MOMENTUM_COEF = 0.95
LEARN_RATE = 0.05
WEIGHT_DECAY = 0.2
NORM_EPS = 1e-7
COEF_A = 3.4445
COEF_B = -4.7750
COEF_C = 2.0315
NS_ITERS = 5
F32 = jnp.float32
BF16 = jnp.bfloat16


def muon_kernel(G, R, g_ref, w_ref, m_ref, wn_ref, mn_ref,
                rl, orl, fo, fi, dr, po, ow, mi, mb, mr, nso, nr, xo, orr, wi, a_s, b_s,
                s_rl, s_fi, s_dr, s_po, s_mr, s_nr, s_or,
                t_raw, t_fo, t_m, t_n, t_o,
                l_rl, l_ow, l_m, l_w):
    NM = G
    RB = mi.shape[2]
    H = RB // 2
    C = mi.shape[3]
    scale = 0.2 * math.sqrt(max(G * RB, C))
    chips = G // 2
    d = lax.axis_index('data')
    p = d // 2
    c = lax.rem(d, 2)
    right = lax.rem(p + 1, chips)
    left = lax.rem(p + chips - 1, chips)
    opp = lax.rem(p + 2, chips)
    partner = 2 * p + (1 - c)

    def remote(src, dst, ssem, rsem, dev):
        pltpu.make_async_remote_copy(src_ref=src, dst_ref=dst, send_sem=ssem, recv_sem=rsem,
                                     device_id={'data': dev}, device_id_type=pl.DeviceIdType.MESH).start()

    def drain(ref, sem):
        pltpu.make_async_copy(ref, ref, sem).wait()

    def mats(r):
        return pl.ds(r * NM, NM)

    def grows(r, dev, half):
        return g_ref.at[mats(r), pl.ds(pl.multiple_of(dev * RB + half * H, H), H), :]

    def load_relay(r):
        s = r % 2
        pltpu.make_async_copy(grows(r, 2 * right + c, 0), orl.at[s, 0], l_rl.at[r]).start()
        pltpu.make_async_copy(grows(r, 2 * left + c, 1), orl.at[s, 1], l_rl.at[r]).start()

    def load_final(r):
        s = r % 2
        pltpu.make_async_copy(g_ref.at[mats(r), pl.ds(pl.multiple_of(d * RB, RB), RB), :], ow.at[s], l_ow.at[r]).start()
        pltpu.make_async_copy(m_ref.at[mats(r)], mi.at[s], l_m.at[r]).start()

    def load_w(r):
        pltpu.make_async_copy(w_ref.at[mats(r)], wi.at[r % 2], l_w.at[r]).start()

    def raw(r):
        for cc in range(2):
            remote(grows(r, 2 * opp + cc, 0), rl.at[r, 0, c], t_raw.at[r], s_rl.at[r, 0], 2 * right + cc)
            remote(grows(r, 2 * opp + cc, 1), rl.at[r, 1, c], t_raw.at[r], s_rl.at[r, 1], 2 * left + cc)
        remote(grows(r, 2 * right + (1 - c), 0), rl.at[r, 0, 2], t_raw.at[r], s_rl.at[r, 0], partner)
        remote(grows(r, 2 * left + (1 - c), 1), rl.at[r, 1, 2], t_raw.at[r], s_rl.at[r, 1], partner)
        for cc in range(2):
            remote(grows(r, 2 * right + cc, 1), dr.at[r, 0, c], t_raw.at[r], s_dr.at[r], 2 * right + cc)
            remote(grows(r, 2 * left + cc, 0), dr.at[r, 1, c], t_raw.at[r], s_dr.at[r], 2 * left + cc)
        remote(g_ref.at[mats(r), pl.ds(pl.multiple_of(partner * RB, RB), RB), :], po.at[r], t_raw.at[r], s_po.at[r], partner)

    def relay(r):
        s = r % 2
        drain(orl.at[s], l_rl.at[r])
        for q in range(2):
            drain(rl.at[r, q], s_rl.at[r, q])
            if r >= 2:
                drain(fo.at[s, q], t_fo.at[r - 2, q])

            def body(k, _):
                fo[s, q, k] = ((rl[r, q, 0, k].astype(F32) + rl[r, q, 1, k].astype(F32))
                               + (rl[r, q, 2, k].astype(F32) + orl[s, q, k].astype(F32)))
                return 0
            lax.fori_loop(0, NM, body, 0)
            remote(fo.at[s, q], fi.at[r, q], t_fo.at[r, q], s_fi.at[r, q], 2 * (right if q == 0 else left) + c)
        if r + 2 < R:
            load_relay(r + 2)

    def final(r):
        s = r % 2
        drain(ow.at[s], l_ow.at[r])
        drain(mi.at[s], l_m.at[r])
        drain(po.at[r], s_po.at[r])
        drain(dr.at[r], s_dr.at[r])
        for q in range(2):
            drain(fi.at[r, q], s_fi.at[r, q])

        def body(k, _):
            part = jnp.zeros((8, 128), F32)
            for q in range(2):
                rows = pl.ds(q * H, H)
                grad = ((dr[r, 1 - q, 0, k].astype(F32) + dr[r, 1 - q, 1, k].astype(F32))
                        + (po[r, k, rows, :].astype(F32) + ow[s, k, rows, :].astype(F32))) + fi[r, q, k]
                new = MOMENTUM_COEF * mi[s, k, rows, :] + grad
                mn_ref[r * NM + k, rows, :] = new
                mb[r, k, rows, :] = new.astype(BF16)
                sq = jnp.sum((new * new).reshape(H // 8, 8, C), axis=0)
                for j in range(C // 128):
                    part = part + sq[:, j * 128:(j + 1) * 128]
            nso[r, k] = jnp.sum(part, axis=0, keepdims=True)
            return 0
        lax.fori_loop(0, NM, body, 0)
        mine = pl.ds(pl.multiple_of(d * RB, RB), RB)
        for j in range(1, G):
            dev = lax.rem(d + j, G)
            remote(nso.at[r, dev], nr.at[r, d], t_n.at[r], s_nr.at[r], dev)
            remote(mb.at[r, dev], mr.at[r, mine, :], t_m.at[r], s_mr.at[r], dev)
        mr[r, mine, :] = mb[r, d]
        nr[r, d] = nso[r, d]
        if r + 2 < R:
            load_final(r + 2)

    def ns(r):
        drain(nr.at[r, pl.ds(0, G - 1)], s_nr.at[r])
        drain(mr.at[r, pl.ds(0, (G - 1) * RB), :], s_mr.at[r])
        tot = jnp.sum(jnp.sum(nr[r], axis=0), axis=(0, 1), keepdims=True)
        denom = jnp.sqrt(tot) + NORM_EPS

        def init(k, _):
            rows = pl.ds(pl.multiple_of(k * RB, RB), RB)
            xo[r, rows, :] = (mr[r, rows, :].astype(F32) / denom).astype(BF16)
            return 0
        lax.fori_loop(0, G, init, 0)

        def step(_, carry):
            x = xo[r]
            a_s[...] = lax.dot_general(x, x, (((1,), (1,)), ((), ())), preferred_element_type=F32).astype(BF16)
            a = a_s[...]
            b_s[...] = (COEF_B * a.astype(F32) + COEF_C * jnp.dot(a, a, preferred_element_type=F32)).astype(BF16)
            xo[r] = (COEF_A * x.astype(F32) + jnp.dot(b_s[...], x, preferred_element_type=F32)).astype(BF16)
            return carry
        lax.fori_loop(0, NS_ITERS, step, 0)

    def osend(r):
        for j in range(1, G):
            dev = lax.rem(d + j, G)
            remote(xo.at[r, pl.ds(pl.multiple_of(dev * RB, RB), RB), :], orr.at[r, d], t_o.at[r], s_or.at[r], dev)
        orr[r, d] = xo[r, pl.ds(pl.multiple_of(d * RB, RB), RB), :]

    def wupd(r):
        s = r % 2
        drain(wi.at[s], l_w.at[r])
        drain(orr.at[r, pl.ds(0, G - 1)], s_or.at[r])

        def body(k, _):
            w = wi[s, k]
            wn_ref[r * NM + k] = w - LEARN_RATE * (orr[r, k].astype(F32) * scale + WEIGHT_DECAY * w)
            return 0
        lax.fori_loop(0, NM, body, 0)
        if r + 2 < R:
            load_w(r + 2)

    bar = pltpu.get_barrier_semaphore()
    for j in range(1, G):
        pl.semaphore_signal(bar, inc=1, device_id={'data': lax.rem(d + j, G)}, device_id_type=pl.DeviceIdType.MESH)
    pl.semaphore_wait(bar, G - 1)

    for r in range(min(2, R)):
        raw(r)
        load_relay(r)
        load_final(r)
        load_w(r)
    for r in range(R):
        relay(r)
        if r + 2 < R:
            raw(r + 2)
        if r >= 1:
            final(r - 1)
        if r >= 2:
            ns(r - 2)
            if r < R - 1:
                osend(r - 2)
        if r >= 3:
            wupd(r - 3)
    final(R - 1)
    osend(R - 3)
    ns(R - 2)
    osend(R - 2)
    wupd(R - 3)
    ns(R - 1)
    osend(R - 1)
    wupd(R - 2)
    wupd(R - 1)
    for r in range(R):
        drain(g_ref.at[pl.ds(0, 6)], t_raw.at[r])
        drain(mb.at[r, pl.ds(0, G - 1)], t_m.at[r])
        drain(nso.at[r, pl.ds(0, G - 1)], t_n.at[r])
        drain(xo.at[r, pl.ds(0, (G - 1) * RB), :], t_o.at[r])
        if r >= R - 2:
            for q in range(2):
                drain(fo.at[r % 2, q], t_fo.at[r, q])


def store_kernel(parts, a_ref, b_ref, ao_ref, bo_ref, sem):
    n = a_ref.shape[0] // parts
    copies = []
    for i in range(parts):
        for j, (src, dst) in enumerate(((a_ref, ao_ref), (b_ref, bo_ref))):
            copies.append(pltpu.make_async_copy(src.at[pl.ds(i * n, n)], dst.at[pl.ds(i * n, n)], sem.at[j, i]))
    for cp in copies:
        cp.start()
    for cp in copies:
        cp.wait()


def solution(mesh):
    G = mesh.shape['data']
    row_spec = P('stage', 'data', None)
    grad_spec = P(('stage', 'data'), None, None, None)

    def local_step(w_rows, mom_rows, grad_full):
        n_mats, RB, C = w_rows.shape
        NM = G
        R = n_mats // NM
        H = RB // 2
        N = G * RB
        assert R * NM == n_mats and grad_full.shape[1:] == (n_mats, N, C) and N == C and G == 8
        dma = pltpu.SemaphoreType.DMA
        vm = pltpu.VMEM
        any_spec = pl.BlockSpec(memory_space=pl.ANY)
        out = vm(w_rows.shape, F32)
        vm_spec = pl.BlockSpec(memory_space=vm)
        w_new, mom_new = pl.pallas_call(
            functools.partial(muon_kernel, G, R),
            out_shape=(out, out),
            in_specs=[any_spec] * 3,
            out_specs=(vm_spec, vm_spec),
            scratch_shapes=[
                vm((R, 2, 3, NM, H, C), BF16),
                vm((2, 2, NM, H, C), BF16),
                vm((2, 2, NM, H, C), F32),
                vm((R, 2, NM, H, C), F32),
                vm((R, 2, 2, NM, H, C), BF16),
                vm((R, NM, RB, C), BF16),
                vm((2, NM, RB, C), BF16),
                vm((2, NM, RB, C), F32),
                vm((R, NM, RB, C), BF16),
                vm((R, N, C), BF16),
                vm((R, NM, 1, 128), F32),
                vm((R, NM, 1, 128), F32),
                vm((R, N, C), BF16),
                vm((R, NM, RB, C), BF16),
                vm((2, NM, RB, C), F32),
                vm((N, N), BF16),
                vm((N, N), BF16),
                dma((R, 2)), dma((R, 2)), dma((R,)), dma((R,)), dma((R,)), dma((R,)), dma((R,)),
                dma((R,)), dma((R, 2)), dma((R,)), dma((R,)), dma((R,)),
                dma((R,)), dma((R,)), dma((R,)), dma((R,)),
            ],
            compiler_params=pltpu.CompilerParams(collective_id=0, has_side_effects=True, vmem_limit_bytes=50 * 2 ** 20),
            cost_estimate=pl.CostEstimate(flops=R * NS_ITERS * 6 * N * N * C, bytes_accessed=100 * 2 ** 20, transcendentals=0),
            name='muon',
        )(grad_full[0], w_rows, mom_rows)
        parts = R
        full = jax.ShapeDtypeStruct(w_rows.shape, F32)
        return pl.pallas_call(
            functools.partial(store_kernel, parts),
            out_shape=(full, full),
            in_specs=[vm_spec, vm_spec],
            out_specs=(any_spec, any_spec),
            scratch_shapes=[dma((2, parts))],
            compiler_params=pltpu.CompilerParams(vmem_limit_bytes=2 ** 20),
            name='store',
        )(w_new, mom_new)

    return jax.shard_map(local_step, mesh=mesh, in_specs=(row_spec, row_spec, grad_spec), out_specs=(row_spec, row_spec), check_vma=False)
```

```python
import functools
import math
import jax
import jax.numpy as jnp
from jax import lax
from jax.experimental import pallas as pl
from jax.experimental.pallas import tpu as pltpu
from jax.sharding import PartitionSpec as P

MOMENTUM_COEF = 0.95
LEARN_RATE = 0.05
WEIGHT_DECAY = 0.2
NORM_EPS = 1e-7
COEF_A = 3.4445
COEF_B = -4.7750
COEF_C = 2.0315
NS_ITERS = 5
STORE_PARTS = 3
ORDER = (
    ('hop', 0), ('direct', 0), ('load', 0), ('load', 1), ('direct', 1), ('relay', 0), ('hop', 1), ('direct', 2), ('relay', 1),
    ('direct', 3), ('hop', 2), ('direct', 4), ('hop', 3), ('hop', 4), ('final', 0), ('relay', 2), ('final', 1), ('relay', 3),
    ('ns', 0), ('relay', 4), ('ns', 1), ('osend', 0), ('hop', 5), ('w', 0), ('osend', 1), ('final', 2), ('direct', 5),
    ('final', 3), ('relay', 5), ('ns', 2), ('w', 1), ('final', 4), ('ns', 3), ('osend', 2), ('final', 5), ('osend', 3),
    ('ns', 4), ('osend', 4), ('w', 2), ('ns', 5), ('osend', 5), ('w', 3), ('w', 4), ('w', 5),
)
F32 = jnp.float32
BF16 = jnp.bfloat16


def muon_kernel(G, R, g_ref, w_ref, m_ref, wn_ref, mn_ref,
                rl, orl, fo, fi, dr, po, ow, mi, mb, mr, nso, nr, xo, orr, wi, a_s, b_s,
                s_rl, s_fi, s_dr, s_po, s_mr, s_nr, s_or,
                t_raw, t_fo, t_m, t_n, t_o,
                l_rl, l_ow, l_m, l_w):
    NM = G
    RB = mi.shape[2]
    H = RB // 2
    C = mi.shape[3]
    scale = 0.2 * math.sqrt(max(G * RB, C))
    chips = G // 2
    d = lax.axis_index('data')
    p = d // 2
    c = lax.rem(d, 2)
    right = lax.rem(p + 1, chips)
    left = lax.rem(p + chips - 1, chips)
    opp = lax.rem(p + 2, chips)
    partner = 2 * p + (1 - c)
    others = (2 * opp, 2 * opp + 1, 2 * right, 2 * left, 2 * right + 1, 2 * left + 1, partner)

    def remote(src, dst, ssem, rsem, dev):
        pltpu.make_async_remote_copy(src_ref=src, dst_ref=dst, send_sem=ssem, recv_sem=rsem,
                                     device_id={'data': dev}, device_id_type=pl.DeviceIdType.MESH).start()

    def drain(ref, sem):
        pltpu.make_async_copy(ref, ref, sem).wait()

    def mats(r):
        return pl.ds(r * NM, NM)

    def grows(r, dev, half):
        return g_ref.at[mats(r), pl.ds(pl.multiple_of(dev * RB + half * H, H), H), :]

    def load_relay(r):
        s = r % 2
        pltpu.make_async_copy(grows(r, 2 * right + c, 0), orl.at[s, 0], l_rl.at[r]).start()
        pltpu.make_async_copy(grows(r, 2 * left + c, 1), orl.at[s, 1], l_rl.at[r]).start()

    def load_final(r):
        s = r % 2
        pltpu.make_async_copy(g_ref.at[mats(r), pl.ds(pl.multiple_of(d * RB, RB), RB), :], ow.at[s], l_ow.at[r]).start()
        pltpu.make_async_copy(m_ref.at[mats(r)], mi.at[s], l_m.at[r]).start()

    def load_w(r):
        pltpu.make_async_copy(w_ref.at[mats(r)], wi.at[r % 2], l_w.at[r]).start()

    def load(r):
        load_relay(r)
        load_final(r)
        load_w(r)

    def raw_hop(r):
        for cc in range(2):
            remote(grows(r, 2 * opp + cc, 0), rl.at[r, 0, c], t_raw.at[r], s_rl.at[r, 0], 2 * right + cc)
            remote(grows(r, 2 * opp + cc, 1), rl.at[r, 1, c], t_raw.at[r], s_rl.at[r, 1], 2 * left + cc)
        remote(grows(r, 2 * right + (1 - c), 0), rl.at[r, 0, 2], t_raw.at[r], s_rl.at[r, 0], partner)
        remote(grows(r, 2 * left + (1 - c), 1), rl.at[r, 1, 2], t_raw.at[r], s_rl.at[r, 1], partner)

    def raw_direct(r):
        for cc in range(2):
            remote(grows(r, 2 * right + cc, 1), dr.at[r, 0, c], t_raw.at[r], s_dr.at[r], 2 * right + cc)
            remote(grows(r, 2 * left + cc, 0), dr.at[r, 1, c], t_raw.at[r], s_dr.at[r], 2 * left + cc)
        remote(g_ref.at[mats(r), pl.ds(pl.multiple_of(partner * RB, RB), RB), :], po.at[r], t_raw.at[r], s_po.at[r], partner)

    def relay(r):
        s = r % 2
        drain(orl.at[s], l_rl.at[r])
        for q in range(2):
            drain(rl.at[r, q], s_rl.at[r, q])
            if r >= 2:
                drain(fo.at[s, q], t_fo.at[r - 2, q])

            def body(k, _):
                fo[s, q, k] = ((rl[r, q, 0, k].astype(F32) + rl[r, q, 1, k].astype(F32))
                               + (rl[r, q, 2, k].astype(F32) + orl[s, q, k].astype(F32)))
                return 0
            lax.fori_loop(0, NM, body, 0)
            remote(fo.at[s, q], fi.at[r, q], t_fo.at[r, q], s_fi.at[r, q], 2 * (right if q == 0 else left) + c)
        if r + 2 < R:
            load_relay(r + 2)

    def final(r):
        s = r % 2
        drain(ow.at[s], l_ow.at[r])
        drain(mi.at[s], l_m.at[r])
        drain(po.at[r], s_po.at[r])
        drain(dr.at[r], s_dr.at[r])
        for q in range(2):
            drain(fi.at[r, q], s_fi.at[r, q])

        def body(k, _):
            part = jnp.zeros((8, 128), F32)
            for q in range(2):
                rows = pl.ds(q * H, H)
                grad = ((dr[r, 1 - q, 0, k].astype(F32) + dr[r, 1 - q, 1, k].astype(F32))
                        + (po[r, k, rows, :].astype(F32) + ow[s, k, rows, :].astype(F32))) + fi[r, q, k]
                new = MOMENTUM_COEF * mi[s, k, rows, :] + grad
                mn_ref[r * NM + k, rows, :] = new
                mb[r, k, rows, :] = new.astype(BF16)
                sq = jnp.sum((new * new).reshape(H // 8, 8, C), axis=0)
                for j in range(C // 128):
                    part = part + sq[:, j * 128:(j + 1) * 128]
            nso[r, k] = jnp.sum(part, axis=0, keepdims=True)
            return 0
        lax.fori_loop(0, NM, body, 0)
        mine = pl.ds(pl.multiple_of(d * RB, RB), RB)
        for dev in others:
            remote(nso.at[r, dev], nr.at[r, d], t_n.at[r], s_nr.at[r], dev)
            remote(mb.at[r, dev], mr.at[r, mine, :], t_m.at[r], s_mr.at[r], dev)
        mr[r, mine, :] = mb[r, d]
        nr[r, d] = nso[r, d]
        if r + 2 < R:
            load_final(r + 2)

    def ns(r):
        drain(nr.at[r, pl.ds(0, G - 1)], s_nr.at[r])
        drain(mr.at[r, pl.ds(0, (G - 1) * RB), :], s_mr.at[r])
        tot = jnp.sum(jnp.sum(nr[r], axis=0), axis=(0, 1), keepdims=True)
        denom = jnp.sqrt(tot) + NORM_EPS

        def init(k, _):
            rows = pl.ds(pl.multiple_of(k * RB, RB), RB)
            xo[r, rows, :] = (mr[r, rows, :].astype(F32) / denom).astype(BF16)
            return 0
        lax.fori_loop(0, G, init, 0)

        def step(_, carry):
            x = xo[r]
            a_s[...] = lax.dot_general(x, x, (((1,), (1,)), ((), ())), preferred_element_type=F32).astype(BF16)
            a = a_s[...]
            b_s[...] = (COEF_B * a.astype(F32) + COEF_C * jnp.dot(a, a, preferred_element_type=F32)).astype(BF16)
            xo[r] = (COEF_A * x.astype(F32) + jnp.dot(b_s[...], x, preferred_element_type=F32)).astype(BF16)
            return carry
        lax.fori_loop(0, NS_ITERS, step, 0)

    def osend(r):
        for dev in others:
            remote(xo.at[r, pl.ds(pl.multiple_of(dev * RB, RB), RB), :], orr.at[r, d], t_o.at[r], s_or.at[r], dev)
        orr[r, d] = xo[r, pl.ds(pl.multiple_of(d * RB, RB), RB), :]

    def wupd(r):
        s = r % 2
        drain(wi.at[s], l_w.at[r])
        drain(orr.at[r, pl.ds(0, G - 1)], s_or.at[r])

        def body(k, _):
            w = wi[s, k]
            wn_ref[r * NM + k] = w - LEARN_RATE * (orr[r, k].astype(F32) * scale + WEIGHT_DECAY * w)
            return 0
        lax.fori_loop(0, NM, body, 0)
        if r + 2 < R:
            load_w(r + 2)

    bar = pltpu.get_barrier_semaphore()
    for j in range(1, G):
        pl.semaphore_signal(bar, inc=1, device_id={'data': lax.rem(d + j, G)}, device_id_type=pl.DeviceIdType.MESH)
    pl.semaphore_wait(bar, G - 1)

    ops = dict(hop=raw_hop, direct=raw_direct, load=load, relay=relay, final=final, ns=ns, osend=osend, w=wupd)
    for name, r in ORDER:
        ops[name](r)
    for r in range(R):
        drain(g_ref.at[pl.ds(0, 6)], t_raw.at[r])
        drain(mb.at[r, pl.ds(0, G - 1)], t_m.at[r])
        drain(nso.at[r, pl.ds(0, G - 1)], t_n.at[r])
        drain(xo.at[r, pl.ds(0, (G - 1) * RB), :], t_o.at[r])
        if r >= R - 2:
            for q in range(2):
                drain(fo.at[r % 2, q], t_fo.at[r, q])


def store_kernel(parts, a_ref, b_ref, ao_ref, bo_ref, sem):
    n = a_ref.shape[0] // parts
    copies = []
    for i in range(parts):
        for j, (src, dst) in enumerate(((a_ref, ao_ref), (b_ref, bo_ref))):
            copies.append(pltpu.make_async_copy(src.at[pl.ds(i * n, n)], dst.at[pl.ds(i * n, n)], sem.at[j, i]))
    for cp in copies:
        cp.start()
    for cp in copies:
        cp.wait()


def solution(mesh):
    G = mesh.shape['data']
    row_spec = P('stage', 'data', None)
    grad_spec = P(('stage', 'data'), None, None, None)

    def local_step(w_rows, mom_rows, grad_full):
        n_mats, RB, C = w_rows.shape
        NM = G
        R = n_mats // NM
        H = RB // 2
        N = G * RB
        assert R * NM == n_mats and grad_full.shape[1:] == (n_mats, N, C) and N == C and G == 8
        assert sorted(r for name, r in ORDER if name == 'w') == list(range(R))
        dma = pltpu.SemaphoreType.DMA
        vm = pltpu.VMEM
        any_spec = pl.BlockSpec(memory_space=pl.ANY)
        out = vm(w_rows.shape, F32)
        vm_spec = pl.BlockSpec(memory_space=vm)
        w_new, mom_new = pl.pallas_call(
            functools.partial(muon_kernel, G, R),
            out_shape=(out, out),
            in_specs=[any_spec] * 3,
            out_specs=(vm_spec, vm_spec),
            scratch_shapes=[
                vm((R, 2, 3, NM, H, C), BF16),
                vm((2, 2, NM, H, C), BF16),
                vm((2, 2, NM, H, C), F32),
                vm((R, 2, NM, H, C), F32),
                vm((R, 2, 2, NM, H, C), BF16),
                vm((R, NM, RB, C), BF16),
                vm((2, NM, RB, C), BF16),
                vm((2, NM, RB, C), F32),
                vm((R, NM, RB, C), BF16),
                vm((R, N, C), BF16),
                vm((R, NM, 1, 128), F32),
                vm((R, NM, 1, 128), F32),
                vm((R, N, C), BF16),
                vm((R, NM, RB, C), BF16),
                vm((2, NM, RB, C), F32),
                vm((N, N), BF16),
                vm((N, N), BF16),
                dma((R, 2)), dma((R, 2)), dma((R,)), dma((R,)), dma((R,)), dma((R,)), dma((R,)),
                dma((R,)), dma((R, 2)), dma((R,)), dma((R,)), dma((R,)),
                dma((R,)), dma((R,)), dma((R,)), dma((R,)),
            ],
            compiler_params=pltpu.CompilerParams(collective_id=0, has_side_effects=True, vmem_limit_bytes=50 * 2 ** 20),
            cost_estimate=pl.CostEstimate(flops=R * NS_ITERS * 6 * N * N * C, bytes_accessed=100 * 2 ** 20, transcendentals=0),
            name='muon',
        )(grad_full[0], w_rows, mom_rows)
        full = jax.ShapeDtypeStruct(w_rows.shape, F32)
        return pl.pallas_call(
            functools.partial(store_kernel, STORE_PARTS),
            out_shape=(full, full),
            in_specs=[vm_spec, vm_spec],
            out_specs=(any_spec, any_spec),
            scratch_shapes=[dma((2, STORE_PARTS))],
            compiler_params=pltpu.CompilerParams(vmem_limit_bytes=2 ** 20),
            name='store',
        )(w_new, mom_new)

    return jax.shard_map(local_step, mesh=mesh, in_specs=(row_spec, row_spec, grad_spec), out_specs=(row_spec, row_spec), check_vma=False)
```

```python
import functools
import math
import jax
import jax.numpy as jnp
from jax import lax
from jax.experimental import pallas as pl
from jax.experimental.pallas import tpu as pltpu
from jax.sharding import PartitionSpec as P

MOMENTUM_COEF = 0.95
LEARN_RATE = 0.05
WEIGHT_DECAY = 0.2
NORM_EPS = 1e-7
COEF_A = 3.4445
COEF_B = -4.7750
COEF_C = 2.0315
NS_ITERS = 5
STORE_PARTS = 3
NORM_SENDS = {1: 2, 3: 2, 4: 1, 5: 1}
ORDER = (
    ('hop', 0), ('direct', 0), ('load', 0), ('load', 1), ('direct', 1), ('relay', 0), ('hop', 1), ('direct', 2), ('relay', 1),
    ('direct', 3), ('hop', 2), ('direct', 4), ('hop', 3), ('hop', 4), ('final', 0), ('relay', 2), ('final', 1), ('relay', 3),
    ('ns', 0), ('relay', 4), ('ns', 1), ('osend', 0), ('hop', 5), ('w', 0), ('osend', 1), ('final', 2), ('direct', 5),
    ('final', 3), ('relay', 5), ('ns', 2), ('w', 1), ('final', 4), ('ns', 3), ('osend', 2), ('final', 5), ('osend', 3),
    ('ns', 4), ('osend', 4), ('w', 2), ('ns', 5), ('osend', 5), ('w', 3), ('w', 4), ('w', 5),
)
F32 = jnp.float32
BF16 = jnp.bfloat16


def weight_step(w, x, scale):
    return w - LEARN_RATE * (x.astype(F32) * scale + WEIGHT_DECAY * w)


def muon_kernel(G, R, g_ref, w_ref, m_ref, wn_ref, mn_ref, wl_ref, xl_ref,
                rl, orl, fo, fi, dr, po, ow, mi, mb, mr, nso, nr, xo, orr, wi, a_s, b_s,
                s_rl, s_fi, s_dr, s_po, s_mr, s_nr, s_or,
                t_raw, t_fo, t_m, t_n, t_o,
                l_rl, l_ow, l_m, l_w, stage, l_st):
    NM = G
    RB = mi.shape[2]
    H = RB // 2
    C = mi.shape[3]
    scale = 0.2 * math.sqrt(max(G * RB, C))
    chips = G // 2
    d = lax.axis_index('data')
    p = d // 2
    c = lax.rem(d, 2)
    right = lax.rem(p + 1, chips)
    left = lax.rem(p + chips - 1, chips)
    opp = lax.rem(p + 2, chips)
    partner = 2 * p + (1 - c)
    others = (2 * opp, 2 * opp + 1, 2 * right, 2 * left, 2 * right + 1, 2 * left + 1, partner)

    def remote(src, dst, ssem, rsem, dev):
        pltpu.make_async_remote_copy(src_ref=src, dst_ref=dst, send_sem=ssem, recv_sem=rsem,
                                     device_id={'data': dev}, device_id_type=pl.DeviceIdType.MESH).start()

    def drain(ref, sem):
        pltpu.make_async_copy(ref, ref, sem).wait()

    def mats(r):
        return pl.ds(r * NM, NM)

    def grows(r, dev, half):
        return g_ref.at[mats(r), pl.ds(pl.multiple_of(dev * RB + half * H, H), H), :]

    def load_relay(r):
        s = r % 2
        pltpu.make_async_copy(grows(r, 2 * right + c, 0), orl.at[s, 0], l_rl.at[r]).start()
        pltpu.make_async_copy(grows(r, 2 * left + c, 1), orl.at[s, 1], l_rl.at[r]).start()

    def load_final(r):
        s = r % 2
        pltpu.make_async_copy(g_ref.at[mats(r), pl.ds(pl.multiple_of(d * RB, RB), RB), :], ow.at[s], l_ow.at[r]).start()
        pltpu.make_async_copy(m_ref.at[mats(r)], mi.at[s], l_m.at[r]).start()

    def load_w(r):
        dst = wl_ref if r == R - 1 else wi.at[r % 2]
        pltpu.make_async_copy(w_ref.at[mats(r)], dst, l_w.at[r]).start()

    def load(r):
        load_relay(r)
        load_final(r)
        load_w(r)

    def raw_hop(r):
        for cc in range(2):
            for q, side in ((0, right), (1, left)):
                rows = stage.at[q] if r == 0 and cc == 0 else grows(r, 2 * opp + cc, q)
                remote(rows, rl.at[r, q, c], t_raw.at[r], s_rl.at[r, q], 2 * side + cc)
        remote(grows(r, 2 * right + (1 - c), 0), rl.at[r, 0, 2], t_raw.at[r], s_rl.at[r, 0], partner)
        remote(grows(r, 2 * left + (1 - c), 1), rl.at[r, 1, 2], t_raw.at[r], s_rl.at[r, 1], partner)

    def raw_direct(r):
        for cc in range(2):
            remote(grows(r, 2 * right + cc, 1), dr.at[r, 0, c], t_raw.at[r], s_dr.at[r], 2 * right + cc)
            remote(grows(r, 2 * left + cc, 0), dr.at[r, 1, c], t_raw.at[r], s_dr.at[r], 2 * left + cc)
        remote(g_ref.at[mats(r), pl.ds(pl.multiple_of(partner * RB, RB), RB), :], po.at[r], t_raw.at[r], s_po.at[r], partner)

    def relay(r):
        s = r % 2
        drain(orl.at[s], l_rl.at[r])
        for q in range(2):
            drain(rl.at[r, q], s_rl.at[r, q])
            if r >= 2:
                drain(fo.at[s, q], t_fo.at[r - 2, q])

            def body(k, _):
                fo[s, q, k] = ((rl[r, q, 0, k].astype(F32) + rl[r, q, 1, k].astype(F32))
                               + (rl[r, q, 2, k].astype(F32) + orl[s, q, k].astype(F32)))
                return 0
            lax.fori_loop(0, NM, body, 0)
            remote(fo.at[s, q], fi.at[r, q], t_fo.at[r, q], s_fi.at[r, q], 2 * (right if q == 0 else left) + c)
        if r + 2 < R:
            load_relay(r + 2)

    def final(r):
        s = r % 2
        drain(ow.at[s], l_ow.at[r])
        drain(mi.at[s], l_m.at[r])
        drain(po.at[r], s_po.at[r])
        drain(dr.at[r], s_dr.at[r])
        for q in range(2):
            drain(fi.at[r, q], s_fi.at[r, q])

        def body(k, _):
            part = jnp.zeros((8, 128), F32)
            for q in range(2):
                rows = pl.ds(q * H, H)
                grad = ((dr[r, 1 - q, 0, k].astype(F32) + dr[r, 1 - q, 1, k].astype(F32))
                        + (po[r, k, rows, :].astype(F32) + ow[s, k, rows, :].astype(F32))) + fi[r, q, k]
                new = MOMENTUM_COEF * mi[s, k, rows, :] + grad
                mn_ref[r * NM + k, rows, :] = new
                mb[r, k, rows, :] = new.astype(BF16)
                sq = jnp.sum((new * new).reshape(H // 8, 8, C), axis=0)
                for j in range(C // 128):
                    part = part + sq[:, j * 128:(j + 1) * 128]
            nso[k, r] = jnp.sum(part, axis=0, keepdims=True)
            return 0
        lax.fori_loop(0, NM, body, 0)
        mine = pl.ds(pl.multiple_of(d * RB, RB), RB)
        for dev in others:
            if r in NORM_SENDS:
                batch = pl.ds(r + 1 - NORM_SENDS[r], NORM_SENDS[r])
                remote(nso.at[dev, batch], nr.at[d, batch], t_n.at[r], s_nr.at[r], dev)
            remote(mb.at[r, dev], mr.at[r, mine, :], t_m.at[r], s_mr.at[r], dev)
        mr[r, mine, :] = mb[r, d]
        nr[d, r] = nso[d, r]
        if r + 2 < R:
            load_final(r + 2)

    def ns(r):
        for q in NORM_SENDS:
            if q + 1 - NORM_SENDS[q] == r:
                drain(nr.at[pl.ds(0, G - 1), pl.ds(0, NORM_SENDS[q])], s_nr.at[q])
        drain(mr.at[r, pl.ds(0, (G - 1) * RB), :], s_mr.at[r])
        tot = jnp.sum(jnp.sum(nr[:, r], axis=0), axis=(0, 1), keepdims=True)
        denom = jnp.sqrt(tot) + NORM_EPS

        def init(k, _):
            rows = pl.ds(pl.multiple_of(k * RB, RB), RB)
            xo[r, rows, :] = (mr[r, rows, :].astype(F32) / denom).astype(BF16)
            return 0
        lax.fori_loop(0, G, init, 0)

        def step(_, carry):
            x = xo[r]
            a_s[...] = lax.dot_general(x, x, (((1,), (1,)), ((), ())), preferred_element_type=F32).astype(BF16)
            a = a_s[...]
            b_s[...] = (COEF_B * a.astype(F32) + COEF_C * jnp.dot(a, a, preferred_element_type=F32)).astype(BF16)
            xo[r] = (COEF_A * x.astype(F32) + jnp.dot(b_s[...], x, preferred_element_type=F32)).astype(BF16)
            return carry
        lax.fori_loop(0, NS_ITERS, step, 0)

    def osend(r):
        for dev in others:
            remote(xo.at[r, pl.ds(pl.multiple_of(dev * RB, RB), RB), :], orr.at[r, d], t_o.at[r], s_or.at[r], dev)
        orr[r, d] = xo[r, pl.ds(pl.multiple_of(d * RB, RB), RB), :]

    def wupd(r):
        s = r % 2
        drain(wl_ref if r == R - 1 else wi.at[s], l_w.at[r])
        drain(orr.at[r, pl.ds(0, G - 1)], s_or.at[r])

        def body(k, _):
            if r == R - 1:
                xl_ref[k] = orr[r, k]
            else:
                wn_ref[r * NM + k] = weight_step(wi[s, k], orr[r, k], scale)
            return 0
        lax.fori_loop(0, NM, body, 0)
        if r + 2 < R:
            load_w(r + 2)

    for q in range(2):
        pltpu.make_async_copy(grows(0, 2 * opp, q), stage.at[q], l_st).start()
    bar = pltpu.get_barrier_semaphore()
    peers = (2 * right, 2 * right + 1, 2 * left, 2 * left + 1, partner)
    for dev in peers:
        pl.semaphore_signal(bar, inc=1, device_id={'data': dev}, device_id_type=pl.DeviceIdType.MESH)
    pl.semaphore_wait(bar, len(peers))
    drain(stage, l_st)

    ops = dict(hop=raw_hop, direct=raw_direct, load=load, relay=relay, final=final, ns=ns, osend=osend, w=wupd)
    for name, r in ORDER:
        ops[name](r)
    for r in range(R):
        drain(g_ref.at[pl.ds(0, 6)], t_raw.at[r])
        drain(mb.at[r, pl.ds(0, G - 1)], t_m.at[r])
        if r in NORM_SENDS:
            drain(nso.at[pl.ds(0, G - 1), pl.ds(0, NORM_SENDS[r])], t_n.at[r])
        drain(xo.at[r, pl.ds(0, (G - 1) * RB), :], t_o.at[r])
        if r >= R - 2:
            for q in range(2):
                drain(fo.at[r % 2, q], t_fo.at[r, q])


def store_kernel(scale, w_ref, m_ref, wl_ref, xl_ref, wo_ref, mo_ref, last, sem, last_sem):
    copies = []
    for j, (src, dst) in enumerate(((m_ref, mo_ref), (w_ref, wo_ref))):
        n = src.shape[0]
        for i in range(STORE_PARTS):
            rows = pl.ds(n * i // STORE_PARTS, n * (i + 1) // STORE_PARTS - n * i // STORE_PARTS)
            copies.append(pltpu.make_async_copy(src.at[rows], dst.at[rows], sem.at[j, i]))
    for cp in copies:
        cp.start()

    def body(k, _):
        last[k] = weight_step(wl_ref[k], xl_ref[k], scale)
        return 0
    lax.fori_loop(0, last.shape[0], body, 0)
    cp = pltpu.make_async_copy(last, wo_ref.at[pl.ds(w_ref.shape[0], last.shape[0])], last_sem)
    cp.start()
    for cp in copies + [cp]:
        cp.wait()


def solution(mesh):
    G = mesh.shape['data']
    row_spec = P('stage', 'data', None)
    grad_spec = P(('stage', 'data'), None, None, None)

    def local_step(w_rows, mom_rows, grad_full):
        n_mats, RB, C = w_rows.shape
        NM = G
        R = n_mats // NM
        H = RB // 2
        N = G * RB
        assert R * NM == n_mats and grad_full.shape[1:] == (n_mats, N, C) and N == C and G == 8
        assert sorted(r for name, r in ORDER if name == 'w') == list(range(R))
        dma = pltpu.SemaphoreType.DMA
        vm = pltpu.VMEM
        any_spec = pl.BlockSpec(memory_space=pl.ANY)
        out = (vm(((R - 1) * NM, RB, C), F32), vm(w_rows.shape, F32), vm((NM, RB, C), F32), vm((NM, RB, C), BF16))
        vm_spec = pl.BlockSpec(memory_space=vm)
        results = pl.pallas_call(
            functools.partial(muon_kernel, G, R),
            out_shape=out,
            in_specs=[any_spec] * 3,
            out_specs=(vm_spec,) * 4,
            scratch_shapes=[
                vm((R, 2, 3, NM, H, C), BF16),
                vm((2, 2, NM, H, C), BF16),
                vm((2, 2, NM, H, C), F32),
                vm((R, 2, NM, H, C), F32),
                vm((R, 2, 2, NM, H, C), BF16),
                vm((R, NM, RB, C), BF16),
                vm((2, NM, RB, C), BF16),
                vm((2, NM, RB, C), F32),
                vm((R, NM, RB, C), BF16),
                vm((R, N, C), BF16),
                vm((G, R, 1, 128), F32),
                vm((G, R, 1, 128), F32),
                vm((R, N, C), BF16),
                vm((R, NM, RB, C), BF16),
                vm((2, NM, RB, C), F32),
                vm((N, N), BF16),
                vm((N, N), BF16),
                dma((R, 2)), dma((R, 2)), dma((R,)), dma((R,)), dma((R,)), dma((R,)), dma((R,)),
                dma((R,)), dma((R, 2)), dma((R,)), dma((R,)), dma((R,)),
                dma((R,)), dma((R,)), dma((R,)), dma((R,)),
                vm((2, NM, H, C), BF16), dma(()),
            ],
            compiler_params=pltpu.CompilerParams(collective_id=0, has_side_effects=True, vmem_limit_bytes=50 * 2 ** 20),
            cost_estimate=pl.CostEstimate(flops=R * NS_ITERS * 6 * N * N * C, bytes_accessed=100 * 2 ** 20, transcendentals=0),
            name='muon',
        )(grad_full[0], w_rows, mom_rows)
        full = jax.ShapeDtypeStruct(w_rows.shape, F32)
        return pl.pallas_call(
            functools.partial(store_kernel, 0.2 * math.sqrt(max(N, C))),
            out_shape=(full, full),
            in_specs=[vm_spec] * 4,
            out_specs=(any_spec, any_spec),
            scratch_shapes=[vm((NM, RB, C), F32), dma((2, STORE_PARTS)), dma(())],
            compiler_params=pltpu.CompilerParams(vmem_limit_bytes=2 ** 21),
            name='store',
        )(*results)

    return jax.shard_map(local_step, mesh=mesh, in_specs=(row_spec, row_spec, grad_spec), out_specs=(row_spec, row_spec), check_vma=False)
```

```python
import functools
import math
import jax
import jax.numpy as jnp
from jax import lax
from jax.experimental import pallas as pl
from jax.experimental.pallas import tpu as pltpu
from jax.sharding import PartitionSpec as P

MOMENTUM_COEF = 0.95
LEARN_RATE = 0.05
WEIGHT_DECAY = 0.2
NORM_EPS = 1e-7
COEF_A = 3.4445
COEF_B = -4.7750
COEF_C = 2.0315
NS_ITERS = 5
STORE_PARTS = 3
NORM_SENDS = {1: 2, 3: 2, 4: 1, 5: 1}
ORDER = (
    ('hop', 0), ('direct', 0), ('load', 0), ('load', 1), ('direct', 1), ('relay', 0), ('hop', 1), ('direct', 2), ('relay', 1),
    ('direct', 3), ('hop', 2), ('direct', 4), ('hop', 3), ('hop', 4), ('final', 0), ('relay', 2), ('final', 1), ('relay', 3),
    ('ns', 0), ('relay', 4), ('ns', 1), ('osend', 0), ('hop', 5), ('w', 0), ('osend', 1), ('final', 2), ('direct', 5),
    ('final', 3), ('relay', 5), ('ns', 2), ('w', 1), ('final', 4), ('ns', 3), ('osend', 2), ('final', 5), ('osend', 3),
    ('ns', 4), ('osend', 4), ('w', 2), ('ns', 5), ('osend', 5), ('w', 3), ('w', 4), ('w', 5),
)
F32 = jnp.float32
BF16 = jnp.bfloat16


def weight_step(w, x, scale):
    return w - LEARN_RATE * (x.astype(F32) * scale + WEIGHT_DECAY * w)


def muon_kernel(G, R, g_ref, w_ref, m_ref, wn_ref, mn_ref, wl_ref, xl_ref,
                rl, orl, fo, fi, dr, po, ow, mi, mb, mr, nso, nr, xo, orr, wi, a_s, b_s,
                s_rl, s_fi, s_dr, s_po, s_mr, s_nr, s_or,
                t_raw, t_fo, t_m, t_n, t_o,
                l_rl, l_ow, l_m, l_w):
    NM = G
    RB = mi.shape[2]
    H = RB // 2
    C = mi.shape[3]
    scale = 0.2 * math.sqrt(max(G * RB, C))
    chips = G // 2
    d = lax.axis_index('data')
    p = d // 2
    c = lax.rem(d, 2)
    right = lax.rem(p + 1, chips)
    left = lax.rem(p + chips - 1, chips)
    opp = lax.rem(p + 2, chips)
    partner = 2 * p + (1 - c)
    others = (2 * opp + 1, 2 * right + 1, 2 * left + 1, 2 * opp, 2 * right, 2 * left, partner)

    def remote(src, dst, ssem, rsem, dev):
        pltpu.make_async_remote_copy(src_ref=src, dst_ref=dst, send_sem=ssem, recv_sem=rsem,
                                     device_id={'data': dev}, device_id_type=pl.DeviceIdType.MESH).start()

    def drain(ref, sem):
        pltpu.make_async_copy(ref, ref, sem).wait()

    def mats(r):
        return pl.ds(r * NM, NM)

    def grows(r, dev, half):
        return g_ref.at[mats(r), pl.ds(pl.multiple_of(dev * RB + half * H, H), H), :]

    def load_relay(r):
        s = r % 2
        pltpu.make_async_copy(grows(r, 2 * right + c, 0), orl.at[s, 0], l_rl.at[r]).start()
        pltpu.make_async_copy(grows(r, 2 * left + c, 1), orl.at[s, 1], l_rl.at[r]).start()

    def load_final(r):
        s = r % 2
        pltpu.make_async_copy(g_ref.at[mats(r), pl.ds(pl.multiple_of(d * RB, RB), RB), :], ow.at[s], l_ow.at[r]).start()
        pltpu.make_async_copy(m_ref.at[mats(r)], mi.at[s], l_m.at[r]).start()

    def load_w(r):
        dst = wl_ref if r == R - 1 else wi.at[r % 2]
        pltpu.make_async_copy(w_ref.at[mats(r)], dst, l_w.at[r]).start()

    def load(r):
        load_relay(r)
        load_final(r)
        load_w(r)

    def raw_hop(r):
        for cc in range(2):
            for q, side in ((0, right), (1, left)):
                rows = grows(r, 2 * opp + cc, q)
                remote(rows, rl.at[r, q, c], t_raw.at[r], s_rl.at[r, q], 2 * side + cc)
        remote(grows(r, 2 * right + (1 - c), 0), rl.at[r, 0, 2], t_raw.at[r], s_rl.at[r, 0], partner)
        remote(grows(r, 2 * left + (1 - c), 1), rl.at[r, 1, 2], t_raw.at[r], s_rl.at[r, 1], partner)

    def raw_direct(r):
        for cc in range(2):
            remote(grows(r, 2 * right + cc, 1), dr.at[r, 0, c], t_raw.at[r], s_dr.at[r], 2 * right + cc)
            remote(grows(r, 2 * left + cc, 0), dr.at[r, 1, c], t_raw.at[r], s_dr.at[r], 2 * left + cc)
        remote(g_ref.at[mats(r), pl.ds(pl.multiple_of(partner * RB, RB), RB), :], po.at[r], t_raw.at[r], s_po.at[r], partner)

    def relay(r):
        s = r % 2
        drain(orl.at[s], l_rl.at[r])
        for q in range(2):
            drain(rl.at[r, q], s_rl.at[r, q])
            if r >= 2:
                drain(fo.at[s, q], t_fo.at[r - 2, q])

            def body(k, _):
                fo[s, q, k] = ((rl[r, q, 0, k].astype(F32) + rl[r, q, 1, k].astype(F32))
                               + (rl[r, q, 2, k].astype(F32) + orl[s, q, k].astype(F32)))
                return 0
            lax.fori_loop(0, NM, body, 0)
            remote(fo.at[s, q], fi.at[r, q], t_fo.at[r, q], s_fi.at[r, q], 2 * (right if q == 0 else left) + c)
        if r + 2 < R:
            load_relay(r + 2)

    def final(r):
        s = r % 2
        drain(ow.at[s], l_ow.at[r])
        drain(mi.at[s], l_m.at[r])
        drain(po.at[r], s_po.at[r])
        drain(dr.at[r], s_dr.at[r])
        for q in range(2):
            drain(fi.at[r, q], s_fi.at[r, q])

        def body(k, _):
            part = jnp.zeros((8, 128), F32)
            for q in range(2):
                rows = pl.ds(q * H, H)
                grad = ((dr[r, 1 - q, 0, k].astype(F32) + dr[r, 1 - q, 1, k].astype(F32))
                        + (po[r, k, rows, :].astype(F32) + ow[s, k, rows, :].astype(F32))) + fi[r, q, k]
                new = MOMENTUM_COEF * mi[s, k, rows, :] + grad
                mn_ref[r * NM + k, rows, :] = new
                mb[r, k, rows, :] = new.astype(BF16)
                sq = jnp.sum((new * new).reshape(H // 8, 8, C), axis=0)
                for j in range(C // 128):
                    part = part + sq[:, j * 128:(j + 1) * 128]
            nso[k, r] = jnp.sum(part, axis=0, keepdims=True)
            return 0
        lax.fori_loop(0, NM, body, 0)
        mine = pl.ds(pl.multiple_of(d * RB, RB), RB)
        for dev in others:
            if r in NORM_SENDS:
                batch = pl.ds(r + 1 - NORM_SENDS[r], NORM_SENDS[r])
                remote(nso.at[dev, batch], nr.at[d, batch], t_n.at[r], s_nr.at[r], dev)
            remote(mb.at[r, dev], mr.at[r, mine, :], t_m.at[r], s_mr.at[r], dev)
        mr[r, mine, :] = mb[r, d]
        nr[d, r] = nso[d, r]
        if r + 2 < R:
            load_final(r + 2)

    def ns(r):
        for q in NORM_SENDS:
            if q + 1 - NORM_SENDS[q] == r:
                drain(nr.at[pl.ds(0, G - 1), pl.ds(0, NORM_SENDS[q])], s_nr.at[q])
        drain(mr.at[r, pl.ds(0, (G - 1) * RB), :], s_mr.at[r])
        tot = jnp.sum(jnp.sum(nr[:, r], axis=0), axis=(0, 1), keepdims=True)
        denom = jnp.sqrt(tot) + NORM_EPS

        def init(k, _):
            rows = pl.ds(pl.multiple_of(k * RB, RB), RB)
            xo[r, rows, :] = (mr[r, rows, :].astype(F32) / denom).astype(BF16)
            return 0
        lax.fori_loop(0, G, init, 0)

        def step(_, carry):
            x = xo[r]
            a_s[...] = lax.dot_general(x, x, (((1,), (1,)), ((), ())), preferred_element_type=F32).astype(BF16)
            a = a_s[...]
            b_s[...] = (COEF_B * a.astype(F32) + COEF_C * jnp.dot(a, a, preferred_element_type=F32)).astype(BF16)
            xo[r] = (COEF_A * x.astype(F32) + jnp.dot(b_s[...], x, preferred_element_type=F32)).astype(BF16)
            return carry
        lax.fori_loop(0, NS_ITERS, step, 0)

    def osend(r):
        for dev in others:
            remote(xo.at[r, pl.ds(pl.multiple_of(dev * RB, RB), RB), :], (xl_ref if r == R - 1 else orr.at[r]).at[d], t_o.at[r], s_or.at[r], dev)
        own = xo[r, pl.ds(pl.multiple_of(d * RB, RB), RB), :]
        if r == R - 1:
            xl_ref[d] = own
        else:
            orr[r, d] = own

    def wupd(r):
        s = r % 2
        drain(wl_ref if r == R - 1 else wi.at[s], l_w.at[r])
        drain((xl_ref if r == R - 1 else orr.at[r]).at[pl.ds(0, G - 1)], s_or.at[r])
        if r == R - 1:
            return

        def body(k, _):
            wn_ref[r * NM + k] = weight_step(wi[s, k], orr[r, k], scale)
            return 0
        lax.fori_loop(0, NM, body, 0)
        if r + 2 < R:
            load_w(r + 2)

    bar = pltpu.get_barrier_semaphore()
    peers = (2 * right, 2 * right + 1, 2 * left, 2 * left + 1, partner)
    for dev in peers:
        pl.semaphore_signal(bar, inc=1, device_id={'data': dev}, device_id_type=pl.DeviceIdType.MESH)
    pl.semaphore_wait(bar, len(peers))

    ops = dict(hop=raw_hop, direct=raw_direct, load=load, relay=relay, final=final, ns=ns, osend=osend, w=wupd)
    for name, r in ORDER:
        ops[name](r)
    for r in range(R):
        drain(g_ref.at[pl.ds(0, 6)], t_raw.at[r])
        drain(mb.at[r, pl.ds(0, G - 1)], t_m.at[r])
        if r in NORM_SENDS:
            drain(nso.at[pl.ds(0, G - 1), pl.ds(0, NORM_SENDS[r])], t_n.at[r])
        drain(xo.at[r, pl.ds(0, (G - 1) * RB), :], t_o.at[r])
        if r >= R - 2:
            for q in range(2):
                drain(fo.at[r % 2, q], t_fo.at[r, q])


def store_kernel(scale, w_ref, m_ref, wl_ref, xl_ref, wo_ref, mo_ref, last, sem, last_sem):
    copies = []
    for j, (src, dst) in enumerate(((m_ref, mo_ref), (w_ref, wo_ref))):
        n = src.shape[0]
        for i in range(STORE_PARTS):
            rows = pl.ds(n * i // STORE_PARTS, n * (i + 1) // STORE_PARTS - n * i // STORE_PARTS)
            copies.append(pltpu.make_async_copy(src.at[rows], dst.at[rows], sem.at[j, i]))
    for cp in copies:
        cp.start()

    def body(k, _):
        last[k] = weight_step(wl_ref[k], xl_ref[k], scale)
        return 0
    lax.fori_loop(0, last.shape[0], body, 0)
    cp = pltpu.make_async_copy(last, wo_ref.at[pl.ds(w_ref.shape[0], last.shape[0])], last_sem)
    cp.start()
    for cp in copies + [cp]:
        cp.wait()


def solution(mesh):
    G = mesh.shape['data']
    row_spec = P('stage', 'data', None)
    grad_spec = P(('stage', 'data'), None, None, None)

    def local_step(w_rows, mom_rows, grad_full):
        n_mats, RB, C = w_rows.shape
        NM = G
        R = n_mats // NM
        H = RB // 2
        N = G * RB
        assert R * NM == n_mats and grad_full.shape[1:] == (n_mats, N, C) and N == C and G == 8
        assert sorted(r for name, r in ORDER if name == 'w') == list(range(R))
        dma = pltpu.SemaphoreType.DMA
        vm = pltpu.VMEM
        any_spec = pl.BlockSpec(memory_space=pl.ANY)
        out = (vm(((R - 1) * NM, RB, C), F32), vm(w_rows.shape, F32), vm((NM, RB, C), F32), vm((NM, RB, C), BF16))
        vm_spec = pl.BlockSpec(memory_space=vm)
        results = pl.pallas_call(
            functools.partial(muon_kernel, G, R),
            out_shape=out,
            in_specs=[any_spec] * 3,
            out_specs=(vm_spec,) * 4,
            scratch_shapes=[
                vm((R, 2, 3, NM, H, C), BF16),
                vm((2, 2, NM, H, C), BF16),
                vm((2, 2, NM, H, C), F32),
                vm((R, 2, NM, H, C), F32),
                vm((R, 2, 2, NM, H, C), BF16),
                vm((R, NM, RB, C), BF16),
                vm((2, NM, RB, C), BF16),
                vm((2, NM, RB, C), F32),
                vm((R, NM, RB, C), BF16),
                vm((R, N, C), BF16),
                vm((G, R, 1, 128), F32),
                vm((G, R, 1, 128), F32),
                vm((R, N, C), BF16),
                vm((R, NM, RB, C), BF16),
                vm((2, NM, RB, C), F32),
                vm((N, N), BF16),
                vm((N, N), BF16),
                dma((R, 2)), dma((R, 2)), dma((R,)), dma((R,)), dma((R,)), dma((R,)), dma((R,)),
                dma((R,)), dma((R, 2)), dma((R,)), dma((R,)), dma((R,)),
                dma((R,)), dma((R,)), dma((R,)), dma((R,)),
            ],
            compiler_params=pltpu.CompilerParams(collective_id=0, has_side_effects=True, vmem_limit_bytes=50 * 2 ** 20),
            cost_estimate=pl.CostEstimate(flops=R * NS_ITERS * 6 * N * N * C, bytes_accessed=100 * 2 ** 20, transcendentals=0),
            name='muon',
        )(grad_full[0], w_rows, mom_rows)
        full = jax.ShapeDtypeStruct(w_rows.shape, F32)
        return pl.pallas_call(
            functools.partial(store_kernel, 0.2 * math.sqrt(max(N, C))),
            out_shape=(full, full),
            in_specs=[vm_spec] * 4,
            out_specs=(any_spec, any_spec),
            scratch_shapes=[vm((NM, RB, C), F32), dma((2, STORE_PARTS)), dma(())],
            compiler_params=pltpu.CompilerParams(vmem_limit_bytes=2 ** 21),
            name='store',
        )(*results)

    return jax.shard_map(local_step, mesh=mesh, in_specs=(row_spec, row_spec, grad_spec), out_specs=(row_spec, row_spec), check_vma=False)
```
